512 devices in a mesh: seq: 16 (over y, core), exp: 32 (over x, z).
Axes of the slice: x: 4, y: 8, z: 8, core: 2. Of those that a mesh axis runs over, the one named last changes fastest.
Arguments:
- tokens: bfloat16 [65536, 1280], P(('seq', 'exp')), may hold values from -64 to 64
- slot_keys: bfloat16 [1280, 32], P(None, 'exp'), may hold values from -3 to 3
- w_in: bfloat16 [32, 5120, 1280], P('exp', 'seq'), may hold values from -0.15625 to 0.15625
- w_out: bfloat16 [32, 5120, 1280], P('exp', 'seq'), may hold values from -0.078125 to 0.078125
- cotangent: bfloat16 [65536, 1280], P(('seq', 'exp')), may hold values from -6 to 6
Outputs:
- layer_out: bfloat16 [65536, 1280], P(('seq', 'exp'))
- tokens_grad: bfloat16 [65536, 1280], P(('seq', 'exp'))
- keys_grad: float32 [1280, 32], P(None, 'exp')
- w_in_grad: bfloat16 [32, 5120, 1280], P('exp', 'seq')
- w_out_grad: bfloat16 [32, 5120, 1280], P('exp', 'seq')
The draws below stay inside these ranges and needn't reach their ends.
All inputs are finite; a program needn't handle non-finite values.
Results may differ from the reference program's by a relative error of at most 0.03.
Values may be sent and summed in bfloat16 or wider, within the bound.
A program may use at most 64 MiB of HBM per device.

```python
import math
import jax
import jax.numpy as jnp
from jax import lax

D = 1280
FF = 5120
EXPERTS = 32
TOKENS = 65536


def slot_table(key):
    sub_key = jax.random.fold_in(key, 7)
    normals = jax.random.truncated_normal(sub_key, -6.0, 6.0, (D, EXPERTS), jnp.float32)
    return normals * (3.0 / math.sqrt(D))


def draw_slot_keys(key, part):
    return slot_table(key).astype(jnp.bfloat16)


def draw_tokens(key, part):
    base_key = jax.random.fold_in(key, 11)
    values = jax.random.truncated_normal(base_key, -6.0, 6.0, (TOKENS, D), jnp.float32)
    return jnp.clip(values, -64.0, 64.0).astype(jnp.bfloat16)


def levels(key, dims, cuts, low, largest):
    level = 1.0
    for dim, blocks in cuts:
        steps = jax.random.uniform(jax.random.fold_in(jax.random.fold_in(key, 6), dim), (blocks,), jnp.float32, low / len(cuts), largest / len(cuts))
        level = level * jnp.repeat(jnp.exp(steps), dims[dim] // blocks).reshape((-1,) + (1,) * (len(dims) - 1 - dim))
    return level


def centred(own_key, extent, width, limit, cuts=(), dtype=jnp.bfloat16):
    factor_of = levels(own_key, extent, cuts, -0.22, 0.18) if cuts else 1.0
    result = jax.random.normal(own_key, extent, jnp.float32) * width * factor_of
    return jnp.minimum(jnp.maximum(result, -limit), limit).astype(dtype)


def setup_inputs(seed: int = 0) -> dict:
    keys = jax.random.split(jax.random.key(seed), 6)
    tokens = draw_tokens(jax.random.fold_in(keys[5], 71), 0)
    slot_keys = draw_slot_keys(jax.random.fold_in(keys[5], 71), 0)
    w_in = centred(keys[2], (EXPERTS, FF, D), D ** -0.5, 0.15625, ((0, 32), (1, 16)))
    w_out = centred(keys[3], (EXPERTS, FF, D), FF ** -0.5, 0.078125, ((0, 32), (1, 16)))
    cotangent = centred(keys[4], (TOKENS, D), 1.0, 6.0, ((0, 512),))
    return dict(tokens=tokens, slot_keys=slot_keys, w_in=w_in, w_out=w_out, cotangent=cotangent)


tanh_coeff = 0.7978845608028654
cubic_coeff = 0.044715


def gelu_value(values):
    return 0.5 * values * (1.0 + jnp.tanh(tanh_coeff * (values + cubic_coeff * values * values * values)))


def gelu_slope(values):
    tanh_part = jnp.tanh(tanh_coeff * (values + cubic_coeff * values * values * values))
    return 0.5 * (1.0 + tanh_part) + 0.5 * values * (1.0 - tanh_part * tanh_part) * tanh_coeff * (1.0 + 3.0 * cubic_coeff * values * values)


def expert_forward(inputs):
    w_first, w_second, slot_row = inputs
    pre_act = jnp.dot(w_first, slot_row, preferred_element_type=jnp.float32)
    activation = gelu_value(pre_act).astype(jnp.bfloat16)
    return pre_act, jnp.dot(activation, w_second, preferred_element_type=jnp.float32)


def expert_backward(inputs):
    w_first, w_second, pre_act, slot_row, grad_row = inputs
    activation = gelu_value(pre_act).astype(jnp.bfloat16)
    act_grad = jnp.dot(w_second, grad_row, preferred_element_type=jnp.float32)
    second_grad = (activation.astype(jnp.float32)[:, None] * grad_row.astype(jnp.float32)[None, :]).astype(jnp.bfloat16)
    pre_grad = (act_grad * gelu_slope(pre_act)).astype(jnp.bfloat16)
    first_grad = (pre_grad.astype(jnp.float32)[:, None] * slot_row.astype(jnp.float32)[None, :]).astype(jnp.bfloat16)
    row_grad = jnp.dot(pre_grad, w_first, preferred_element_type=jnp.float32)
    return first_grad, second_grad, row_grad


def reference(tokens, slot_keys, w_in, w_out, cotangent):
    logits = jnp.dot(tokens, slot_keys, preferred_element_type=jnp.float32)
    slot_peak = jnp.max(logits, axis=0, keepdims=True)
    exp_terms = jnp.exp(logits - slot_peak)
    disp_prob = exp_terms / jnp.sum(exp_terms, axis=0, keepdims=True)
    dispatch = disp_prob.astype(jnp.bfloat16)
    slot_in = jnp.dot(dispatch.T, tokens, preferred_element_type=jnp.float32).astype(jnp.bfloat16)
    pre_act, slot_sum = lax.map(expert_forward, (w_in, w_out, slot_in))
    slot_out = slot_sum.astype(jnp.bfloat16)
    row_peak = jnp.max(logits, axis=1, keepdims=True)
    row_terms = jnp.exp(logits - row_peak)
    comb_prob = row_terms / jnp.sum(row_terms, axis=1, keepdims=True)
    combine = comb_prob.astype(jnp.bfloat16)
    layer_out = jnp.dot(combine, slot_out, preferred_element_type=jnp.float32).astype(jnp.bfloat16)
    comb_grad = jnp.dot(cotangent, slot_out.T, preferred_element_type=jnp.float32)
    slot_out_grad = jnp.dot(combine.T, cotangent, preferred_element_type=jnp.float32).astype(jnp.bfloat16)
    w_in_grad, w_out_grad, row_grads = lax.map(expert_backward, (w_in, w_out, pre_act, slot_in, slot_out_grad))
    slot_in_grad = row_grads.astype(jnp.bfloat16)
    disp_grad = jnp.dot(tokens, slot_in_grad.T, preferred_element_type=jnp.float32)
    correction = jnp.sum(disp_prob * disp_grad, axis=0, keepdims=True)
    comb_mean = jnp.sum(comb_prob * comb_grad, axis=1, keepdims=True)
    logit_grad = (comb_prob * (comb_grad - comb_mean) + disp_prob * (disp_grad - correction)).astype(jnp.bfloat16)
    tokens_grad = (jnp.dot(dispatch, slot_in_grad, preferred_element_type=jnp.float32)
                   + jnp.dot(logit_grad, slot_keys.T, preferred_element_type=jnp.float32)).astype(jnp.bfloat16)
    keys_grad = jnp.dot(tokens.T, logit_grad, preferred_element_type=jnp.float32)
    return layer_out, tokens_grad, keys_grad, w_in_grad, w_out_grad
```

```python
import functools

import jax
import jax.numpy as jnp
from jax import lax
from jax.experimental import pallas as pl
from jax.experimental.pallas import tpu as pltpu
from jax.sharding import PartitionSpec as P

tanh_coeff = 0.7978845608028654
cubic_coeff = 0.044715
F32 = jnp.float32
BF16 = jnp.bfloat16
MESH = pl.DeviceIdType.MESH
LANES = 128


def gelu_value(values):
    return (
        0.5
        * values
        * (1.0 + jnp.tanh(tanh_coeff * (values + cubic_coeff * values * values * values)))
    )


def gelu_slope(values):
    tanh_part = jnp.tanh(tanh_coeff * (values + cubic_coeff * values * values * values))
    return 0.5 * (1.0 + tanh_part) + 0.5 * values * (1.0 - tanh_part * tanh_part) * tanh_coeff * (
        1.0 + 3.0 * cubic_coeff * values * values
    )


def split_in_three(value):
    high = value.astype(BF16).astype(F32)
    rest = value - high
    middle = rest.astype(BF16).astype(F32)
    return high, middle, rest - middle


def packed_scalars(values):
    rows = values[0].shape[0]
    lane = lax.broadcasted_iota(jnp.int32, (rows, LANES), 1)
    result = jnp.zeros((rows, LANES), F32)
    at = 0
    for value in values:
        for part in split_in_three(value):
            result = jnp.where(lane == at, part, result)
            at += 1
    return result


def unpacked_scalars(row, count):
    lane = lax.broadcasted_iota(jnp.int32, row.shape, 1)
    found = []
    for k in range(count):
        mine = (lane >= 3 * k) & (lane < 3 * k + 3)
        found.append(jnp.sum(jnp.where(mine, row, 0.0), axis=1, keepdims=True))
    return found


def high_and_low(value):
    high = value.astype(BF16).astype(F32)
    return high, value - high


def pair_of_rows(row):
    high, low = high_and_low(row)
    at = lax.broadcasted_iota(jnp.int32, (16, 1), 0)
    return jnp.where(at == 0, high, jnp.where(at == 1, low, 0.0)).astype(BF16)


def dot(a, b, dims):
    return lax.dot_general(a, b, (dims, ((), ())), preferred_element_type=F32)


def kernel(
    n_seq, n_exp, x_hbm, keys_hbm, w_in_hbm, w_out_hbm, c_hbm,
    layer_out, tokens_grad, keys_grad, w_in_grad, w_out_grad,
    x, keys_ref, c, w_in, w_out, k_all, so, sg, row_f, flat_f,
    a_buf, c1_send_in, c1_send_grad, c1_in, c1_grad, c2_in, c2_grad,
    e_out, e_grad, f_buf, h1_send, h1_buf, h2_buf,
    load_sem, send_sem, recv_sem,
):
    width = x.shape[1]
    blocks = width // LANES
    pairs = blocks // 2
    tall = blocks + 1
    s_me = lax.axis_index("seq")
    e_me = lax.axis_index("exp")

    loads = [
        pltpu.make_async_copy(source, target, load_sem.at[k])
        for k, (source, target) in enumerate(
            ((x_hbm, x), (c_hbm, c), (w_in_hbm, w_in), (w_out_hbm, w_out), (keys_hbm, keys_ref))
        )
    ]

    barrier = pltpu.get_barrier_semaphore()

    def greet_exp(k, carry):
        pl.semaphore_signal(
            barrier, inc=1, device_id=(s_me, lax.rem(e_me + k, n_exp)), device_id_type=MESH
        )
        return carry

    def greet_seq(k, carry):
        pl.semaphore_signal(
            barrier, inc=1, device_id=(lax.rem(s_me + k, n_seq), e_me), device_id_type=MESH
        )
        return carry

    loads[4].start()
    lax.fori_loop(1, n_exp, greet_exp, 0)
    lax.fori_loop(1, n_seq, greet_seq, 0)
    for load in loads[:4]:
        load.start()

    def exchange(over_exp, *parts):
        n, me = (n_exp, e_me) if over_exp else (n_seq, s_me)

        def send(k, carry):
            peer = lax.rem(me + k, n)
            target = (s_me, peer) if over_exp else (peer, e_me)
            for at, unit, source, buf in parts:
                mine = buf.at[pl.ds(me * unit, unit)]
                pltpu.make_async_remote_copy(
                    src_ref=mine if source is None else source.at[pl.ds(peer * unit, unit)],
                    dst_ref=mine,
                    send_sem=send_sem.at[at],
                    recv_sem=recv_sem.at[at],
                    device_id=target,
                    device_id_type=MESH,
                ).start()
            return carry

        lax.fori_loop(1, n, send, 0)

    def whole(over_exp, at, unit, source, buf):
        n, me = (n_exp, e_me) if over_exp else (n_seq, s_me)
        peer = lax.rem(me + 1, n)
        every = buf.at[pl.ds(0, (n - 1) * unit)]
        return pltpu.make_async_remote_copy(
            src_ref=every,
            dst_ref=every,
            send_sem=send_sem.at[at],
            recv_sem=recv_sem.at[at],
            device_id=(s_me, peer) if over_exp else (peer, e_me),
            device_id_type=MESH,
        )

    started = []

    def begin(over_exp, *parts):
        exchange(over_exp, *parts)
        started.extend(whole(over_exp, *part) for part in parts)

        def arrived():
            for part in parts:
                whole(over_exp, *part).wait_recv()

        return arrived

    def cut(row):
        return [row[:, k * LANES : (k + 1) * LANES] for k in range(blocks)]

    def store_pairs(buf, me, rows):
        for k, row in enumerate(rows):
            row_f[pl.ds(k, 1), :] = row
        count = len(rows)
        unit = count // 2
        buf[pl.ds(me * unit, unit)] = row_f[0:count, :].reshape(unit, 2, LANES).astype(BF16)

    def store_rows(buf, me, unit, rows):
        for k, row in enumerate(rows):
            buf[pl.ds(me * unit + k, 1)] = row.reshape(1, 1, LANES)

    def load_pairs(buf):
        count = buf.shape[0] * 2
        flat_f[0:count, :] = buf.reshape(count, LANES)[...].astype(F32)

    def picked(source, row, count, rows):
        return source[pl.ds(row, count, stride=rows), :]

    def split_to(target, first, rows, values):
        for k in range(blocks):
            target[pl.ds(first + k, n_exp, stride=rows), :] = values[:, k * LANES : (k + 1) * LANES]

    lane = lax.broadcasted_iota(jnp.int32, (1, LANES), 1)

    def two_scalars(a, b):
        return jnp.where(lane < LANES // 2, a, b)

    loads[4].wait()
    store_pairs(a_buf, e_me, cut(keys_ref[...].astype(F32)))
    pl.semaphore_wait(barrier, n_exp - 1 + n_seq - 1)
    arrived = begin(True, (0, pairs, None, a_buf))
    loads[0].wait()
    loads[1].wait()
    arrived()
    load_pairs(a_buf)
    for k in range(blocks):
        k_all[:, k * LANES : (k + 1) * LANES] = picked(flat_f, k, n_exp, blocks).astype(BF16)

    logits = dot(k_all[...], x[...], ((1,), (1,)))
    local_peak = jnp.max(logits, axis=1, keepdims=True)
    local_terms = jnp.exp(logits - local_peak)
    local_total = jnp.sum(local_terms, axis=1, keepdims=True)
    row_peak = jnp.max(logits, axis=0, keepdims=True)
    row_terms = jnp.exp(logits - row_peak)
    comb_prob = row_terms / jnp.sum(row_terms, axis=0, keepdims=True)
    combine = comb_prob.astype(BF16)

    def rows_of(weights, data):
        both = jnp.concatenate(high_and_low(weights), axis=0).astype(BF16)
        result = dot(both, data[...], ((1,), (0,)))
        return result[0:n_exp] + result[n_exp:]

    grad_view = c1_send_grad.reshape(n_exp * tall, LANES)
    grad_view[pl.ds(blocks, n_exp, stride=tall), :] = two_scalars(local_peak, local_total)
    split_to(grad_view, 0, tall, rows_of(comb_prob, c))
    split_to(flat_f, 0, blocks, rows_of(local_terms, x))
    c1_send_in.reshape(n_exp * blocks, LANES)[...] = flat_f[0 : n_exp * blocks, :].astype(BF16)
    c1_grad[pl.ds(e_me * tall, tall)] = c1_send_grad[pl.ds(e_me * tall, tall)]
    c1_in[pl.ds(e_me * pairs, pairs)] = c1_send_in[pl.ds(e_me * pairs, pairs)]
    arrived = begin(True, (1, tall, c1_send_grad, c1_grad), (2, pairs, c1_send_in, c1_in))
    arrived()

    def summed(source, count, rows, scale=None):
        result = []
        for k in range(blocks):
            part = picked(source, k, count, rows)
            if scale is not None:
                part = part * scale
            result.append(jnp.sum(part, axis=0, keepdims=True))
        return result

    def merged(buf_in, buf_grad, count):
        grad = buf_grad.reshape(count * tall, LANES)
        load_pairs(buf_in)
        stats = picked(grad, blocks, count, tall)
        peaks, totals = stats[:, 0:1], stats[:, LANES // 2 : LANES // 2 + 1]
        peak = jnp.max(peaks, axis=0, keepdims=True)
        scale = jnp.exp(peaks - peak)
        total = jnp.sum(scale * totals, axis=0, keepdims=True)
        return summed(flat_f, count, blocks, scale), summed(grad, count, tall), peak, total

    first, second, peak, total = merged(c1_in, c1_grad, n_exp)
    store_rows(c2_grad, s_me, tall, second + [two_scalars(peak, total)])
    store_pairs(c2_in, s_me, first)
    arrived = begin(False, (3, tall, None, c2_grad), (4, pairs, None, c2_in))
    loads[2].wait()
    loads[3].wait()
    arrived()
    first, second, slot_peak, slot_total = merged(c2_in, c2_grad, n_seq)
    slot_in = [part / slot_total for part in first]

    def times(row, matrix, dim):
        result = dot(row, matrix[...], ((1,), (dim,)))
        return result[0:1] + result[1:2]

    in_lhs = pair_of_rows(jnp.concatenate(slot_in, axis=1))
    out_lhs = pair_of_rows(jnp.concatenate(second, axis=1))
    pre_act = times(in_lhs, w_in, 1)
    act_grad = times(out_lhs, w_out, 1)
    activation = gelu_value(pre_act)
    pre_grad = act_grad * gelu_slope(pre_act)
    slot_out_part = times(pair_of_rows(activation), w_out, 0)
    slot_in_grad_part = times(pair_of_rows(pre_grad), w_in, 0)

    store_rows(e_grad, s_me, blocks, cut(slot_in_grad_part))
    store_pairs(e_out, s_me, cut(slot_out_part))
    arrived = begin(False, (5, blocks, None, e_grad), (6, pairs, None, e_out))

    first_row = lax.broadcasted_iota(jnp.int32, (16, 1), 0) == 0
    act_lhs = jnp.where(first_row, activation, 0.0).astype(BF16)
    pre_lhs = jnp.where(first_row, pre_grad, 0.0).astype(BF16)
    step = 2 * LANES
    for k in range(width // step):
        cols = slice(k * step, (k + 1) * step)
        w_out_grad[:, cols] = dot(act_lhs, out_lhs[:, cols], ((0,), (0,))).astype(BF16)
        w_in_grad[:, cols] = dot(pre_lhs, in_lhs[:, cols], ((0,), (0,))).astype(BF16)

    arrived()
    slot_in_grad = summed(e_grad.reshape(n_seq * blocks, LANES), n_seq, blocks)
    load_pairs(e_out)
    slot_out = summed(flat_f, n_seq, blocks)
    products = [a * b.astype(BF16).astype(F32) for a, b in zip(slot_in, slot_in_grad)]
    correction = jnp.sum(functools.reduce(jnp.add, products), axis=1, keepdims=True)

    both = 2 * (blocks + 1)
    scalars = packed_scalars((slot_peak, slot_total, correction))
    store_pairs(f_buf, e_me, slot_out + slot_in_grad + [scalars, jnp.zeros((1, LANES), F32)])
    arrived = begin(True, (7, both // 2, None, f_buf))
    arrived()
    load_pairs(f_buf)
    for k in range(blocks):
        cols = slice(k * LANES, (k + 1) * LANES)
        so[:, cols] = picked(flat_f, k, n_exp, both).astype(BF16)
        sg[:, cols] = picked(flat_f, blocks + k, n_exp, both).astype(BF16)
    peaks, totals, corrections = unpacked_scalars(picked(flat_f, 2 * blocks, n_exp, both), 3)

    comb_grad = dot(so[...], c[...], ((1,), (1,)))
    disp_grad = dot(sg[...], x[...], ((1,), (1,)))
    disp_prob = jnp.exp(logits - peaks) / totals
    comb_mean = jnp.sum(comb_prob * comb_grad, axis=0, keepdims=True)
    logit_grad = (
        comb_prob * (comb_grad - comb_mean) + disp_prob * (disp_grad - corrections)
    ).astype(BF16)

    split_to(flat_f, 0, blocks, dot(logit_grad, x[...], ((1,), (0,))))
    h1_send.reshape(n_exp * blocks, LANES)[...] = flat_f[0 : n_exp * blocks, :].astype(BF16)
    h1_buf[pl.ds(e_me * pairs, pairs)] = h1_send[pl.ds(e_me * pairs, pairs)]
    arrived = begin(True, (8, pairs, h1_send, h1_buf))

    layer_out[...] = dot(combine, so[...], ((0,), (0,))).astype(BF16)
    tokens_grad[...] = (
        dot(disp_prob.astype(BF16), sg[...], ((0,), (0,))) + dot(logit_grad, k_all[...], ((0,), (0,)))
    ).astype(BF16)

    arrived()
    load_pairs(h1_buf)
    store_pairs(h2_buf, s_me, summed(flat_f, n_exp, blocks))

    arrived = begin(False, (9, pairs, None, h2_buf))
    for copies in started:
        copies.wait_send()
    arrived()
    load_pairs(h2_buf)
    for k, part in enumerate(summed(flat_f, n_seq, blocks)):
        keys_grad[:, k * LANES : (k + 1) * LANES] = part


def put_kernel(*refs):
    count = (len(refs) - 1) // 2
    copies = [
        pltpu.make_async_copy(refs[k], refs[count + k], refs[-1].at[k]) for k in range(count)
    ]
    for copy in copies:
        copy.start()
    for copy in copies:
        copy.wait()


def put(arrays):
    count = len(arrays)
    return pl.pallas_call(
        put_kernel,
        out_shape=tuple(pltpu.HBM(a.shape, a.dtype) for a in arrays),
        in_specs=[pl.BlockSpec(memory_space=pltpu.VMEM)] * count,
        out_specs=(pl.BlockSpec(memory_space=pltpu.HBM),) * count,
        scratch_shapes=[pltpu.SemaphoreType.DMA((count,))],
        compiler_params=pltpu.CompilerParams(vmem_limit_bytes=1024 * 1024),
        name="put",
    )(*arrays)


def local(n_seq, n_exp, tokens, slot_keys, w_in, w_out, cotangent):
    rows, width = tokens.shape
    hidden = w_in.shape[1]
    blocks = width // LANES
    pairs = blocks // 2
    tall = blocks + 1

    def pairs_of(count):
        return pltpu.VMEM((count, 2, LANES), BF16)

    def rows_of(count):
        return pltpu.VMEM((count, 1, LANES), F32)

    hbm = pl.BlockSpec(memory_space=pltpu.HBM)
    vmem = pl.BlockSpec(memory_space=pltpu.VMEM)
    layer_out, tokens_grad, keys_grad, w_in_grad, w_out_grad = pl.pallas_call(
        functools.partial(kernel, n_seq, n_exp),
        out_shape=(
            pltpu.VMEM((rows, width), BF16),
            pltpu.VMEM((rows, width), BF16),
            pltpu.VMEM((1, width), F32),
            pltpu.VMEM((hidden, width), BF16),
            pltpu.VMEM((hidden, width), BF16),
        ),
        in_specs=[hbm, hbm, hbm, hbm, hbm],
        out_specs=(vmem, vmem, vmem, vmem, vmem),
        scratch_shapes=[
            pltpu.VMEM((rows, width), BF16),
            pltpu.VMEM((1, width), BF16),
            pltpu.VMEM((rows, width), BF16),
            pltpu.VMEM((hidden, width), BF16),
            pltpu.VMEM((hidden, width), BF16),
            pltpu.VMEM((n_exp, width), BF16),
            pltpu.VMEM((n_exp, width), BF16),
            pltpu.VMEM((n_exp, width), BF16),
            pltpu.VMEM((2 * tall, LANES), F32),
            pltpu.VMEM((max(n_seq, n_exp) * 2 * tall, LANES), F32),
            pairs_of(n_exp * pairs),
            pairs_of(n_exp * pairs),
            rows_of(n_exp * tall),
            pairs_of(n_exp * pairs),
            rows_of(n_exp * tall),
            pairs_of(n_seq * pairs),
            rows_of(n_seq * tall),
            pairs_of(n_seq * pairs),
            rows_of(n_seq * blocks),
            pairs_of(n_exp * tall),
            pairs_of(n_exp * pairs),
            pairs_of(n_exp * pairs),
            pairs_of(n_seq * pairs),
            pltpu.SemaphoreType.DMA((5,)),
            pltpu.SemaphoreType.DMA((10,)),
            pltpu.SemaphoreType.DMA((10,)),
        ],
        compiler_params=pltpu.CompilerParams(
            collective_id=0, has_side_effects=True, vmem_limit_bytes=32 * 1024 * 1024
        ),
        name="moe",
    )(
        *(
            pltpu.with_memory_space_constraint(a, pltpu.HBM)
            for a in (tokens, slot_keys.T, w_in[0], w_out[0], cotangent)
        )
    )
    layer_out, tokens_grad, keys_grad, w_in_grad, w_out_grad = put(
        (layer_out, tokens_grad, keys_grad, w_in_grad, w_out_grad)
    )
    return layer_out, tokens_grad, keys_grad.T, w_in_grad[None], w_out_grad[None]


def solution(mesh):
    n_seq, n_exp = mesh.shape["seq"], mesh.shape["exp"]
    placed = (
        P(("seq", "exp"), None),
        P(None, "exp"),
        P("exp", "seq", None),
        P("exp", "seq", None),
        P(("seq", "exp"), None),
    )
    return jax.shard_map(
        functools.partial(local, n_seq, n_exp),
        mesh=mesh,
        in_specs=placed,
        out_specs=(
            P(("seq", "exp"), None),
            P(("seq", "exp"), None),
            P(None, "exp"),
            P("exp", "seq", None),
            P("exp", "seq", None),
        ),
        check_vma=False,
    )
```

```python
import functools

import jax
import jax.numpy as jnp
from jax import lax
from jax.experimental import pallas as pl
from jax.experimental.pallas import tpu as pltpu
from jax.sharding import PartitionSpec as P

tanh_coeff = 0.7978845608028654
cubic_coeff = 0.044715
F32 = jnp.float32
BF16 = jnp.bfloat16
MESH = pl.DeviceIdType.MESH
LANES = 128


def gelu_value(values):
    return (
        0.5
        * values
        * (1.0 + jnp.tanh(tanh_coeff * (values + cubic_coeff * values * values * values)))
    )


def gelu_slope(values):
    tanh_part = jnp.tanh(tanh_coeff * (values + cubic_coeff * values * values * values))
    return 0.5 * (1.0 + tanh_part) + 0.5 * values * (1.0 - tanh_part * tanh_part) * tanh_coeff * (
        1.0 + 3.0 * cubic_coeff * values * values
    )


def split_in_three(value):
    high = value.astype(BF16).astype(F32)
    rest = value - high
    middle = rest.astype(BF16).astype(F32)
    return high, middle, rest - middle


def packed_scalars(values):
    rows = values[0].shape[0]
    lane = lax.broadcasted_iota(jnp.int32, (rows, LANES), 1)
    result = jnp.zeros((rows, LANES), F32)
    at = 0
    for value in values:
        for part in split_in_three(value):
            result = jnp.where(lane == at, part, result)
            at += 1
    return result


def unpacked_scalars(row, count):
    lane = lax.broadcasted_iota(jnp.int32, row.shape, 1)
    found = []
    for k in range(count):
        mine = (lane >= 3 * k) & (lane < 3 * k + 3)
        found.append(jnp.sum(jnp.where(mine, row, 0.0), axis=1, keepdims=True))
    return found


def high_and_low(value):
    high = value.astype(BF16).astype(F32)
    return high, value - high


def pair_of_rows(row):
    high, low = high_and_low(row)
    at = lax.broadcasted_iota(jnp.int32, (16, 1), 0)
    return jnp.where(at == 0, high, jnp.where(at == 1, low, 0.0)).astype(BF16)


def dot(a, b, dims):
    return lax.dot_general(a, b, (dims, ((), ())), preferred_element_type=F32)


def farthest_first(n, over_exp):
    inner = 8 if over_exp and n % 8 == 0 else n

    def hops(k):
        near, far = k % inner, k // inner
        return min(near, inner - near) + min(far, n // inner - far)

    return sorted(range(1, n), key=lambda k: -hops(k))


def kernel(
    n_seq, n_exp, x_hbm, keys_hbm, w_in_hbm, w_out_hbm, c_hbm,
    layer_out, tokens_grad, keys_grad, w_in_grad, w_out_grad,
    x, keys_ref, c, w_in, w_out, k_all, so, sg, row_f, flat_f,
    a_buf, c1_send_in, c1_send_grad, c1_in, c1_grad, c2_in, c2_grad,
    e_out, e_grad, f_buf, h1_send, h1_buf, h2_buf,
    load_sem, send_sem, recv_sem,
):
    width = x.shape[1]
    blocks = width // LANES
    pairs = blocks // 2
    tall = blocks + 1
    s_me = lax.axis_index("seq")
    e_me = lax.axis_index("exp")

    loads = [
        pltpu.make_async_copy(source, target, load_sem.at[k])
        for k, (source, target) in enumerate(
            ((x_hbm, x), (c_hbm, c), (w_in_hbm, w_in), (w_out_hbm, w_out), (keys_hbm, keys_ref))
        )
    ]

    barrier = pltpu.get_barrier_semaphore()

    def greet_exp(k, carry):
        pl.semaphore_signal(
            barrier, inc=1, device_id=(s_me, lax.rem(e_me + k, n_exp)), device_id_type=MESH
        )
        return carry

    def greet_seq(k, carry):
        pl.semaphore_signal(
            barrier, inc=1, device_id=(lax.rem(s_me + k, n_seq), e_me), device_id_type=MESH
        )
        return carry

    loads[4].start()
    lax.fori_loop(1, n_exp, greet_exp, 0)
    lax.fori_loop(1, n_seq, greet_seq, 0)
    for load in loads[:4]:
        load.start()

    def exchange(over_exp, *parts):
        n, me = (n_exp, e_me) if over_exp else (n_seq, s_me)

        for k in farthest_first(n, over_exp):
            peer = lax.rem(me + k, n)
            target = (s_me, peer) if over_exp else (peer, e_me)
            for at, unit, source, buf in parts:
                mine = buf.at[pl.ds(me * unit, unit)]
                pltpu.make_async_remote_copy(
                    src_ref=mine if source is None else source.at[pl.ds(peer * unit, unit)],
                    dst_ref=mine,
                    send_sem=send_sem.at[at],
                    recv_sem=recv_sem.at[at],
                    device_id=target,
                    device_id_type=MESH,
                ).start()

    def whole(over_exp, at, unit, source, buf):
        n, me = (n_exp, e_me) if over_exp else (n_seq, s_me)
        peer = lax.rem(me + 1, n)
        every = buf.at[pl.ds(0, (n - 1) * unit)]
        return pltpu.make_async_remote_copy(
            src_ref=every,
            dst_ref=every,
            send_sem=send_sem.at[at],
            recv_sem=recv_sem.at[at],
            device_id=(s_me, peer) if over_exp else (peer, e_me),
            device_id_type=MESH,
        )

    started = []

    def begin(over_exp, *parts):
        exchange(over_exp, *parts)
        started.extend(whole(over_exp, *part) for part in parts)

        def arrived():
            for part in parts:
                whole(over_exp, *part).wait_recv()

        return arrived

    def cut(row):
        return [row[:, k * LANES : (k + 1) * LANES] for k in range(blocks)]

    def store_pairs(buf, me, rows):
        for k, row in enumerate(rows):
            row_f[pl.ds(k, 1), :] = row
        count = len(rows)
        unit = count // 2
        buf[pl.ds(me * unit, unit)] = row_f[0:count, :].reshape(unit, 2, LANES).astype(BF16)

    def store_rows(buf, me, unit, rows):
        for k, row in enumerate(rows):
            buf[pl.ds(me * unit + k, 1)] = row.reshape(1, 1, LANES)

    def load_pairs(buf):
        count = buf.shape[0] * 2
        flat_f[0:count, :] = buf.reshape(count, LANES)[...].astype(F32)

    def picked(source, row, count, rows):
        return source[pl.ds(row, count, stride=rows), :]

    def split_to(target, first, rows, values):
        for k in range(blocks):
            target[pl.ds(first + k, n_exp, stride=rows), :] = values[:, k * LANES : (k + 1) * LANES]

    lane = lax.broadcasted_iota(jnp.int32, (1, LANES), 1)

    def two_scalars(a, b):
        return jnp.where(lane < LANES // 2, a, b)

    loads[4].wait()
    store_pairs(a_buf, e_me, cut(keys_ref[...].astype(F32)))
    pl.semaphore_wait(barrier, n_exp - 1 + n_seq - 1)
    arrived = begin(True, (0, pairs, None, a_buf))
    loads[0].wait()
    loads[1].wait()
    arrived()
    load_pairs(a_buf)
    for k in range(blocks):
        k_all[:, k * LANES : (k + 1) * LANES] = picked(flat_f, k, n_exp, blocks).astype(BF16)

    logits = dot(k_all[...], x[...], ((1,), (1,)))
    local_peak = jnp.max(logits, axis=1, keepdims=True)
    local_terms = jnp.exp(logits - local_peak)
    local_total = jnp.sum(local_terms, axis=1, keepdims=True)
    row_peak = jnp.max(logits, axis=0, keepdims=True)
    row_terms = jnp.exp(logits - row_peak)
    comb_prob = row_terms / jnp.sum(row_terms, axis=0, keepdims=True)
    combine = comb_prob.astype(BF16)

    def rows_of(weights, data):
        both = jnp.concatenate(high_and_low(weights), axis=0).astype(BF16)
        result = dot(both, data[...], ((1,), (0,)))
        return result[0:n_exp] + result[n_exp:]

    grad_view = c1_send_grad.reshape(n_exp * tall, LANES)
    grad_view[pl.ds(blocks, n_exp, stride=tall), :] = two_scalars(local_peak, local_total)
    split_to(grad_view, 0, tall, rows_of(comb_prob, c))
    c1_grad[pl.ds(e_me * tall, tall)] = c1_send_grad[pl.ds(e_me * tall, tall)]
    arrived_grad = begin(True, (1, tall, c1_send_grad, c1_grad))
    split_to(flat_f, 0, blocks, rows_of(local_terms, x))
    c1_send_in.reshape(n_exp * blocks, LANES)[...] = flat_f[0 : n_exp * blocks, :].astype(BF16)
    c1_in[pl.ds(e_me * pairs, pairs)] = c1_send_in[pl.ds(e_me * pairs, pairs)]
    arrived = begin(True, (2, pairs, c1_send_in, c1_in))
    arrived_grad()
    arrived()

    def summed(source, count, rows, scale=None):
        result = []
        for k in range(blocks):
            part = picked(source, k, count, rows)
            if scale is not None:
                part = part * scale
            result.append(jnp.sum(part, axis=0, keepdims=True))
        return result

    def merged(buf_in, buf_grad, count):
        grad = buf_grad.reshape(count * tall, LANES)
        load_pairs(buf_in)
        stats = picked(grad, blocks, count, tall)
        peaks, totals = stats[:, 0:1], stats[:, LANES // 2 : LANES // 2 + 1]
        peak = jnp.max(peaks, axis=0, keepdims=True)
        scale = jnp.exp(peaks - peak)
        total = jnp.sum(scale * totals, axis=0, keepdims=True)
        return summed(flat_f, count, blocks, scale), summed(grad, count, tall), peak, total

    first, second, peak, total = merged(c1_in, c1_grad, n_exp)
    store_rows(c2_grad, s_me, tall, second + [two_scalars(peak, total)])
    store_pairs(c2_in, s_me, first)
    arrived = begin(False, (3, tall, None, c2_grad), (4, pairs, None, c2_in))
    loads[2].wait()
    loads[3].wait()
    arrived()
    first, second, slot_peak, slot_total = merged(c2_in, c2_grad, n_seq)
    slot_in = [part / slot_total for part in first]

    def times(row, matrix, dim):
        result = dot(row, matrix[...], ((1,), (dim,)))
        return result[0:1] + result[1:2]

    in_lhs = pair_of_rows(jnp.concatenate(slot_in, axis=1))
    out_lhs = pair_of_rows(jnp.concatenate(second, axis=1))
    pre_act = times(in_lhs, w_in, 1)
    act_grad = times(out_lhs, w_out, 1)
    activation = gelu_value(pre_act)
    pre_grad = act_grad * gelu_slope(pre_act)
    slot_out_part = times(pair_of_rows(activation), w_out, 0)
    slot_in_grad_part = times(pair_of_rows(pre_grad), w_in, 0)

    store_rows(e_grad, s_me, blocks, cut(slot_in_grad_part))
    store_pairs(e_out, s_me, cut(slot_out_part))
    arrived = begin(False, (5, blocks, None, e_grad), (6, pairs, None, e_out))

    first_row = lax.broadcasted_iota(jnp.int32, (16, 1), 0) == 0
    act_lhs = jnp.where(first_row, activation, 0.0).astype(BF16)
    pre_lhs = jnp.where(first_row, pre_grad, 0.0).astype(BF16)
    step = 2 * LANES
    for k in range(width // step):
        cols = slice(k * step, (k + 1) * step)
        w_out_grad[:, cols] = dot(act_lhs, out_lhs[:, cols], ((0,), (0,))).astype(BF16)
        w_in_grad[:, cols] = dot(pre_lhs, in_lhs[:, cols], ((0,), (0,))).astype(BF16)

    arrived()
    slot_in_grad = summed(e_grad.reshape(n_seq * blocks, LANES), n_seq, blocks)
    load_pairs(e_out)
    slot_out = summed(flat_f, n_seq, blocks)
    products = [a * b.astype(BF16).astype(F32) for a, b in zip(slot_in, slot_in_grad)]
    correction = jnp.sum(functools.reduce(jnp.add, products), axis=1, keepdims=True)

    both = 2 * (blocks + 1)
    scalars = packed_scalars((slot_peak, slot_total, correction))
    store_pairs(f_buf, e_me, slot_out + slot_in_grad + [scalars, jnp.zeros((1, LANES), F32)])
    arrived = begin(True, (7, both // 2, None, f_buf))
    arrived()
    load_pairs(f_buf)
    for k in range(blocks):
        cols = slice(k * LANES, (k + 1) * LANES)
        so[:, cols] = picked(flat_f, k, n_exp, both).astype(BF16)
        sg[:, cols] = picked(flat_f, blocks + k, n_exp, both).astype(BF16)
    peaks, totals, corrections = unpacked_scalars(picked(flat_f, 2 * blocks, n_exp, both), 3)

    comb_grad = dot(so[...], c[...], ((1,), (1,)))
    disp_grad = dot(sg[...], x[...], ((1,), (1,)))
    disp_prob = jnp.exp(logits - peaks) / totals
    comb_mean = jnp.sum(comb_prob * comb_grad, axis=0, keepdims=True)
    logit_grad = (
        comb_prob * (comb_grad - comb_mean) + disp_prob * (disp_grad - corrections)
    ).astype(BF16)

    split_to(flat_f, 0, blocks, dot(logit_grad, x[...], ((1,), (0,))))
    h1_send.reshape(n_exp * blocks, LANES)[...] = flat_f[0 : n_exp * blocks, :].astype(BF16)
    h1_buf[pl.ds(e_me * pairs, pairs)] = h1_send[pl.ds(e_me * pairs, pairs)]
    arrived = begin(True, (8, pairs, h1_send, h1_buf))

    layer_out[...] = dot(combine, so[...], ((0,), (0,))).astype(BF16)
    tokens_grad[...] = (
        dot(disp_prob.astype(BF16), sg[...], ((0,), (0,))) + dot(logit_grad, k_all[...], ((0,), (0,)))
    ).astype(BF16)

    arrived()
    load_pairs(h1_buf)
    store_pairs(h2_buf, s_me, summed(flat_f, n_exp, blocks))

    arrived = begin(False, (9, pairs, None, h2_buf))
    for copies in started:
        copies.wait_send()
    arrived()
    load_pairs(h2_buf)
    for k, part in enumerate(summed(flat_f, n_seq, blocks)):
        keys_grad[:, k * LANES : (k + 1) * LANES] = part


def put_kernel(*refs):
    count = (len(refs) - 1) // 2
    copies = []
    for k in range(count):
        rows = refs[k].shape[0]
        parts = 2 if rows % 32 == 0 else 1
        for part in range(parts):
            at = pl.ds(part * (rows // parts), rows // parts)
            copies.append(
                pltpu.make_async_copy(
                    refs[k].at[at], refs[count + k].at[at], refs[-1].at[2 * k + part]
                )
            )
    for copy in copies:
        copy.start()
    for copy in copies:
        copy.wait()


def put(arrays):
    count = len(arrays)
    return pl.pallas_call(
        put_kernel,
        out_shape=tuple(pltpu.HBM(a.shape, a.dtype) for a in arrays),
        in_specs=[pl.BlockSpec(memory_space=pltpu.VMEM)] * count,
        out_specs=(pl.BlockSpec(memory_space=pltpu.HBM),) * count,
        scratch_shapes=[pltpu.SemaphoreType.DMA((2 * count,))],
        compiler_params=pltpu.CompilerParams(vmem_limit_bytes=1024 * 1024),
        name="put",
    )(*arrays)


def local(n_seq, n_exp, tokens, slot_keys, w_in, w_out, cotangent):
    rows, width = tokens.shape
    hidden = w_in.shape[1]
    blocks = width // LANES
    pairs = blocks // 2
    tall = blocks + 1

    def pairs_of(count):
        return pltpu.VMEM((count, 2, LANES), BF16)

    def rows_of(count):
        return pltpu.VMEM((count, 1, LANES), F32)

    hbm = pl.BlockSpec(memory_space=pltpu.HBM)
    vmem = pl.BlockSpec(memory_space=pltpu.VMEM)
    layer_out, tokens_grad, keys_grad, w_in_grad, w_out_grad = pl.pallas_call(
        functools.partial(kernel, n_seq, n_exp),
        out_shape=(
            pltpu.VMEM((rows, width), BF16),
            pltpu.VMEM((rows, width), BF16),
            pltpu.VMEM((1, width), F32),
            pltpu.VMEM((hidden, width), BF16),
            pltpu.VMEM((hidden, width), BF16),
        ),
        in_specs=[hbm, hbm, hbm, hbm, hbm],
        out_specs=(vmem, vmem, vmem, vmem, vmem),
        scratch_shapes=[
            pltpu.VMEM((rows, width), BF16),
            pltpu.VMEM((1, width), BF16),
            pltpu.VMEM((rows, width), BF16),
            pltpu.VMEM((hidden, width), BF16),
            pltpu.VMEM((hidden, width), BF16),
            pltpu.VMEM((n_exp, width), BF16),
            pltpu.VMEM((n_exp, width), BF16),
            pltpu.VMEM((n_exp, width), BF16),
            pltpu.VMEM((2 * tall, LANES), F32),
            pltpu.VMEM((max(n_seq, n_exp) * 2 * tall, LANES), F32),
            pairs_of(n_exp * pairs),
            pairs_of(n_exp * pairs),
            rows_of(n_exp * tall),
            pairs_of(n_exp * pairs),
            rows_of(n_exp * tall),
            pairs_of(n_seq * pairs),
            rows_of(n_seq * tall),
            pairs_of(n_seq * pairs),
            rows_of(n_seq * blocks),
            pairs_of(n_exp * tall),
            pairs_of(n_exp * pairs),
            pairs_of(n_exp * pairs),
            pairs_of(n_seq * pairs),
            pltpu.SemaphoreType.DMA((5,)),
            pltpu.SemaphoreType.DMA((10,)),
            pltpu.SemaphoreType.DMA((10,)),
        ],
        compiler_params=pltpu.CompilerParams(
            collective_id=0, has_side_effects=True, vmem_limit_bytes=32 * 1024 * 1024
        ),
        name="moe",
    )(
        *(
            pltpu.with_memory_space_constraint(a, pltpu.HBM)
            for a in (tokens, slot_keys.T, w_in[0], w_out[0], cotangent)
        )
    )
    layer_out, tokens_grad, keys_grad, w_in_grad, w_out_grad = put(
        (layer_out, tokens_grad, keys_grad, w_in_grad, w_out_grad)
    )
    return layer_out, tokens_grad, keys_grad.T, w_in_grad[None], w_out_grad[None]


def solution(mesh):
    n_seq, n_exp = mesh.shape["seq"], mesh.shape["exp"]
    placed = (
        P(("seq", "exp"), None),
        P(None, "exp"),
        P("exp", "seq", None),
        P("exp", "seq", None),
        P(("seq", "exp"), None),
    )
    return jax.shard_map(
        functools.partial(local, n_seq, n_exp),
        mesh=mesh,
        in_specs=placed,
        out_specs=(
            P(("seq", "exp"), None),
            P(("seq", "exp"), None),
            P(None, "exp"),
            P("exp", "seq", None),
            P("exp", "seq", None),
        ),
        check_vma=False,
    )
```

```python
import functools

import jax
import jax.numpy as jnp
from jax import lax
from jax.experimental import pallas as pl
from jax.experimental.pallas import tpu as pltpu
from jax.sharding import PartitionSpec as P

tanh_coeff = 0.7978845608028654
cubic_coeff = 0.044715
F32 = jnp.float32
BF16 = jnp.bfloat16
MESH = pl.DeviceIdType.MESH
LANES = 128


def gelu_value(values):
    return (
        0.5
        * values
        * (1.0 + jnp.tanh(tanh_coeff * (values + cubic_coeff * values * values * values)))
    )


def gelu_slope(values):
    tanh_part = jnp.tanh(tanh_coeff * (values + cubic_coeff * values * values * values))
    return 0.5 * (1.0 + tanh_part) + 0.5 * values * (1.0 - tanh_part * tanh_part) * tanh_coeff * (
        1.0 + 3.0 * cubic_coeff * values * values
    )


def split_in_three(value):
    high = value.astype(BF16).astype(F32)
    rest = value - high
    middle = rest.astype(BF16).astype(F32)
    return high, middle, rest - middle


def packed_scalars(values):
    rows = values[0].shape[0]
    lane = lax.broadcasted_iota(jnp.int32, (rows, LANES), 1)
    result = jnp.zeros((rows, LANES), F32)
    at = 0
    for value in values:
        for part in split_in_three(value):
            result = jnp.where(lane == at, part, result)
            at += 1
    return result


def unpacked_scalars(row, count):
    lane = lax.broadcasted_iota(jnp.int32, row.shape, 1)
    found = []
    for k in range(count):
        mine = (lane >= 3 * k) & (lane < 3 * k + 3)
        found.append(jnp.sum(jnp.where(mine, row, 0.0), axis=1, keepdims=True))
    return found


def high_and_low(value):
    high = value.astype(BF16).astype(F32)
    return high, value - high


def dot(a, b, dims):
    return lax.dot_general(a, b, (dims, ((), ())), preferred_element_type=F32)


def farthest_first(n, over_exp):
    inner = 8 if over_exp and n % 8 == 0 else n

    def hops(k):
        near, far = k % inner, k // inner
        return min(near, inner - near) + min(far, n // inner - far)

    return sorted(range(1, n), key=lambda k: -hops(k))


def kernel(
    n_seq, n_exp, x_hbm, keys_hbm, w_in_hbm, w_out_hbm, c_hbm,
    layer_out, tokens_grad, keys_grad, w_in_grad, w_out_grad,
    x, keys_ref, c, w_in, w_out, k_all, so, sg, row_f, flat_f,
    a_buf, c1_send_in, c1_send_grad, c1_in, c1_grad, c2_in, c2_grad,
    e_out, e_grad, f_buf, h1_send, h1_buf, h2_buf,
    load_sem, send_sem, recv_sem,
):
    width = x.shape[1]
    blocks = width // LANES
    pairs = blocks // 2
    tall = blocks + 1
    s_me = lax.axis_index("seq")
    e_me = lax.axis_index("exp")

    loads = [
        pltpu.make_async_copy(source, target, load_sem.at[k])
        for k, (source, target) in enumerate(
            ((x_hbm, x), (c_hbm, c), (w_in_hbm, w_in), (w_out_hbm, w_out), (keys_hbm, keys_ref))
        )
    ]

    barrier = pltpu.get_barrier_semaphore()

    loads[4].start()
    for k in farthest_first(n_exp, True):
        pl.semaphore_signal(
            barrier, inc=1, device_id=(s_me, lax.rem(e_me + k, n_exp)), device_id_type=MESH
        )
    for k in farthest_first(n_seq, False):
        pl.semaphore_signal(
            barrier, inc=1, device_id=(lax.rem(s_me + k, n_seq), e_me), device_id_type=MESH
        )
    for load in loads[:4]:
        load.start()

    def exchange(over_exp, *parts):
        n, me = (n_exp, e_me) if over_exp else (n_seq, s_me)

        for k in farthest_first(n, over_exp):
            peer = lax.rem(me + k, n)
            target = (s_me, peer) if over_exp else (peer, e_me)
            for at, unit, source, buf in parts:
                mine = buf.at[pl.ds(me * unit, unit)]
                pltpu.make_async_remote_copy(
                    src_ref=mine if source is None else source.at[pl.ds(peer * unit, unit)],
                    dst_ref=mine,
                    send_sem=send_sem.at[at],
                    recv_sem=recv_sem.at[at],
                    device_id=target,
                    device_id_type=MESH,
                ).start()

    def whole(over_exp, at, unit, source, buf):
        n, me = (n_exp, e_me) if over_exp else (n_seq, s_me)
        peer = lax.rem(me + 1, n)
        every = buf.at[pl.ds(0, (n - 1) * unit)]
        return pltpu.make_async_remote_copy(
            src_ref=every,
            dst_ref=every,
            send_sem=send_sem.at[at],
            recv_sem=recv_sem.at[at],
            device_id=(s_me, peer) if over_exp else (peer, e_me),
            device_id_type=MESH,
        )

    started = []

    def begin(over_exp, *parts):
        exchange(over_exp, *parts)
        started.extend(whole(over_exp, *part) for part in parts)

        def arrived():
            for part in parts:
                whole(over_exp, *part).wait_recv()

        return arrived

    def cut(row):
        return [row[:, k * LANES : (k + 1) * LANES] for k in range(blocks)]

    def store_pairs(buf, me, rows):
        for k, row in enumerate(rows):
            row_f[pl.ds(k, 1), :] = row
        count = len(rows)
        unit = count // 2
        buf[pl.ds(me * unit, unit)] = row_f[0:count, :].reshape(unit, 2, LANES).astype(BF16)

    def store_rows(buf, me, unit, rows):
        for k, row in enumerate(rows):
            buf[pl.ds(me * unit + k, 1)] = row.reshape(1, 1, LANES)

    def load_pairs(buf):
        count = buf.shape[0] * 2
        flat_f[0:count, :] = buf.reshape(count, LANES)[...].astype(F32)

    def picked(source, row, count, rows):
        return source[pl.ds(row, count, stride=rows), :]

    def split_to(target, first, rows, values):
        for k in range(blocks):
            target[pl.ds(first + k, n_exp, stride=rows), :] = values[:, k * LANES : (k + 1) * LANES]

    lane = lax.broadcasted_iota(jnp.int32, (1, LANES), 1)

    def two_scalars(a, b):
        return jnp.where(lane < LANES // 2, a, b)

    loads[4].wait()
    store_pairs(a_buf, e_me, cut(keys_ref[...].astype(F32)))
    pl.semaphore_wait(barrier, n_exp - 1 + n_seq - 1)
    arrived = begin(True, (0, pairs, None, a_buf))
    loads[0].wait()
    loads[1].wait()
    arrived()
    load_pairs(a_buf)
    for k in range(blocks):
        k_all[:, k * LANES : (k + 1) * LANES] = picked(flat_f, k, n_exp, blocks).astype(BF16)

    logits = dot(k_all[...], x[...], ((1,), (1,)))
    local_peak = jnp.max(logits, axis=1, keepdims=True)
    local_terms = jnp.exp(logits - local_peak)
    local_total = jnp.sum(local_terms, axis=1, keepdims=True)
    row_peak = jnp.max(logits, axis=0, keepdims=True)
    row_terms = jnp.exp(logits - row_peak)
    comb_prob = row_terms / jnp.sum(row_terms, axis=0, keepdims=True)
    combine = comb_prob.astype(BF16)

    grad_view = c1_send_grad.reshape(n_exp * tall, LANES)
    grad_view[pl.ds(blocks, n_exp, stride=tall), :] = two_scalars(local_peak, local_total)
    split_to(grad_view, 0, tall, dot(combine, c[...], ((1,), (0,))))
    c1_grad[pl.ds(e_me * tall, tall)] = c1_send_grad[pl.ds(e_me * tall, tall)]
    arrived_grad = begin(True, (1, tall, c1_send_grad, c1_grad))
    both_terms = jnp.concatenate(high_and_low(local_terms), axis=0).astype(BF16)
    in_rows = dot(both_terms, x[...], ((1,), (0,)))
    split_to(flat_f, 0, blocks, in_rows[0:n_exp] + in_rows[n_exp:])
    c1_send_in.reshape(n_exp * blocks, LANES)[...] = flat_f[0 : n_exp * blocks, :].astype(BF16)
    c1_in[pl.ds(e_me * pairs, pairs)] = c1_send_in[pl.ds(e_me * pairs, pairs)]
    arrived = begin(True, (2, pairs, c1_send_in, c1_in))
    arrived_grad()
    arrived()

    def summed(source, count, rows, scale=None):
        result = []
        for k in range(blocks):
            part = picked(source, k, count, rows)
            if scale is not None:
                part = part * scale
            result.append(jnp.sum(part, axis=0, keepdims=True))
        return result

    def merged(buf_in, buf_grad, count):
        grad = buf_grad.reshape(count * tall, LANES)
        load_pairs(buf_in)
        stats = picked(grad, blocks, count, tall)
        peaks, totals = stats[:, 0:1], stats[:, LANES // 2 : LANES // 2 + 1]
        peak = jnp.max(peaks, axis=0, keepdims=True)
        scale = jnp.exp(peaks - peak)
        total = jnp.sum(scale * totals, axis=0, keepdims=True)
        return summed(flat_f, count, blocks, scale), summed(grad, count, tall), peak, total

    first, second, peak, total = merged(c1_in, c1_grad, n_exp)
    store_rows(c2_grad, s_me, tall, second + [two_scalars(peak, total)])
    store_pairs(c2_in, s_me, first)
    arrived = begin(False, (3, tall, None, c2_grad), (4, pairs, None, c2_in))
    loads[2].wait()
    loads[3].wait()
    arrived()
    first, second, slot_peak, slot_total = merged(c2_in, c2_grad, n_seq)
    slot_in = [part / slot_total for part in first]

    in_first = lax.broadcasted_iota(jnp.int32, (16, 1), 0) == 0

    def first_row(row):
        return jnp.where(in_first, row, 0.0).astype(BF16)

    def times(row, matrix, dim):
        return dot(row, matrix[...], ((1,), (dim,)))[0:1]

    in_lhs = first_row(jnp.concatenate(slot_in, axis=1))
    out_lhs = first_row(jnp.concatenate(second, axis=1))
    pre_act = times(in_lhs, w_in, 1)
    act_grad = times(out_lhs, w_out, 1)
    act_lhs = first_row(gelu_value(pre_act))
    pre_lhs = first_row(act_grad * gelu_slope(pre_act))
    slot_in_grad_part = times(pre_lhs, w_in, 0)
    slot_out_part = times(act_lhs, w_out, 0)

    store_rows(e_grad, s_me, blocks, cut(slot_in_grad_part))
    store_pairs(e_out, s_me, cut(slot_out_part))
    arrived = begin(False, (5, blocks, None, e_grad), (6, pairs, None, e_out))

    step = 2 * LANES
    for k in range(width // step):
        cols = slice(k * step, (k + 1) * step)
        w_out_grad[:, cols] = dot(act_lhs, out_lhs[:, cols], ((0,), (0,))).astype(BF16)
        w_in_grad[:, cols] = dot(pre_lhs, in_lhs[:, cols], ((0,), (0,))).astype(BF16)

    arrived()
    slot_in_grad = summed(e_grad.reshape(n_seq * blocks, LANES), n_seq, blocks)
    load_pairs(e_out)
    slot_out = summed(flat_f, n_seq, blocks)
    products = [a * b.astype(BF16).astype(F32) for a, b in zip(slot_in, slot_in_grad)]
    correction = jnp.sum(functools.reduce(jnp.add, products), axis=1, keepdims=True)

    both = 2 * (blocks + 1)
    scalars = packed_scalars((slot_peak, slot_total, correction))
    store_pairs(f_buf, e_me, slot_out + slot_in_grad + [scalars, jnp.zeros((1, LANES), F32)])
    arrived = begin(True, (7, both // 2, None, f_buf))
    arrived()
    load_pairs(f_buf)
    for k in range(blocks):
        cols = slice(k * LANES, (k + 1) * LANES)
        so[:, cols] = picked(flat_f, k, n_exp, both).astype(BF16)
        sg[:, cols] = picked(flat_f, blocks + k, n_exp, both).astype(BF16)
    peaks, totals, corrections = unpacked_scalars(picked(flat_f, 2 * blocks, n_exp, both), 3)

    comb_grad = dot(so[...], c[...], ((1,), (1,)))
    disp_grad = dot(sg[...], x[...], ((1,), (1,)))
    disp_prob = jnp.exp(logits - peaks) / totals
    comb_mean = jnp.sum(comb_prob * comb_grad, axis=0, keepdims=True)
    logit_grad = (
        comb_prob * (comb_grad - comb_mean) + disp_prob * (disp_grad - corrections)
    ).astype(BF16)

    split_to(flat_f, 0, blocks, dot(logit_grad, x[...], ((1,), (0,))))
    h1_send.reshape(n_exp * blocks, LANES)[...] = flat_f[0 : n_exp * blocks, :].astype(BF16)
    h1_buf[pl.ds(e_me * pairs, pairs)] = h1_send[pl.ds(e_me * pairs, pairs)]
    arrived = begin(True, (8, pairs, h1_send, h1_buf))

    layer_out[...] = dot(combine, so[...], ((0,), (0,))).astype(BF16)
    tokens_grad[...] = (
        dot(disp_prob.astype(BF16), sg[...], ((0,), (0,))) + dot(logit_grad, k_all[...], ((0,), (0,)))
    ).astype(BF16)

    arrived()
    load_pairs(h1_buf)
    store_pairs(h2_buf, s_me, summed(flat_f, n_exp, blocks))

    arrived = begin(False, (9, pairs, None, h2_buf))
    for copies in started:
        copies.wait_send()
    arrived()
    load_pairs(h2_buf)
    for k, part in enumerate(summed(flat_f, n_seq, blocks)):
        keys_grad[:, k * LANES : (k + 1) * LANES] = part


def put_kernel(*refs):
    count = (len(refs) - 1) // 2
    copies = []
    for k in range(count):
        rows = refs[k].shape[0]
        parts = 2 if rows % 32 == 0 else 1
        for part in range(parts):
            at = pl.ds(part * (rows // parts), rows // parts)
            copies.append(
                pltpu.make_async_copy(
                    refs[k].at[at], refs[count + k].at[at], refs[-1].at[2 * k + part]
                )
            )
    for copy in copies:
        copy.start()
    for copy in copies:
        copy.wait()


def put(arrays):
    count = len(arrays)
    return pl.pallas_call(
        put_kernel,
        out_shape=tuple(pltpu.HBM(a.shape, a.dtype) for a in arrays),
        in_specs=[pl.BlockSpec(memory_space=pltpu.VMEM)] * count,
        out_specs=(pl.BlockSpec(memory_space=pltpu.HBM),) * count,
        scratch_shapes=[pltpu.SemaphoreType.DMA((2 * count,))],
        compiler_params=pltpu.CompilerParams(vmem_limit_bytes=1024 * 1024),
        name="put",
    )(*arrays)


def local(n_seq, n_exp, tokens, slot_keys, w_in, w_out, cotangent):
    rows, width = tokens.shape
    hidden = w_in.shape[1]
    blocks = width // LANES
    pairs = blocks // 2
    tall = blocks + 1

    def pairs_of(count):
        return pltpu.VMEM((count, 2, LANES), BF16)

    def rows_of(count):
        return pltpu.VMEM((count, 1, LANES), F32)

    hbm = pl.BlockSpec(memory_space=pltpu.HBM)
    vmem = pl.BlockSpec(memory_space=pltpu.VMEM)
    layer_out, tokens_grad, keys_grad, w_in_grad, w_out_grad = pl.pallas_call(
        functools.partial(kernel, n_seq, n_exp),
        out_shape=(
            pltpu.VMEM((rows, width), BF16),
            pltpu.VMEM((rows, width), BF16),
            pltpu.VMEM((1, width), F32),
            pltpu.VMEM((hidden, width), BF16),
            pltpu.VMEM((hidden, width), BF16),
        ),
        in_specs=[hbm, hbm, hbm, hbm, hbm],
        out_specs=(vmem, vmem, vmem, vmem, vmem),
        scratch_shapes=[
            pltpu.VMEM((rows, width), BF16),
            pltpu.VMEM((1, width), BF16),
            pltpu.VMEM((rows, width), BF16),
            pltpu.VMEM((hidden, width), BF16),
            pltpu.VMEM((hidden, width), BF16),
            pltpu.VMEM((n_exp, width), BF16),
            pltpu.VMEM((n_exp, width), BF16),
            pltpu.VMEM((n_exp, width), BF16),
            pltpu.VMEM((2 * tall, LANES), F32),
            pltpu.VMEM((max(n_seq, n_exp) * 2 * tall, LANES), F32),
            pairs_of(n_exp * pairs),
            pairs_of(n_exp * pairs),
            rows_of(n_exp * tall),
            pairs_of(n_exp * pairs),
            rows_of(n_exp * tall),
            pairs_of(n_seq * pairs),
            rows_of(n_seq * tall),
            pairs_of(n_seq * pairs),
            rows_of(n_seq * blocks),
            pairs_of(n_exp * tall),
            pairs_of(n_exp * pairs),
            pairs_of(n_exp * pairs),
            pairs_of(n_seq * pairs),
            pltpu.SemaphoreType.DMA((5,)),
            pltpu.SemaphoreType.DMA((10,)),
            pltpu.SemaphoreType.DMA((10,)),
        ],
        compiler_params=pltpu.CompilerParams(
            collective_id=0, has_side_effects=True, vmem_limit_bytes=32 * 1024 * 1024
        ),
        name="moe",
    )(
        *(
            pltpu.with_memory_space_constraint(a, pltpu.HBM)
            for a in (tokens, slot_keys.T, w_in[0], w_out[0], cotangent)
        )
    )
    layer_out, tokens_grad, keys_grad, w_in_grad, w_out_grad = put(
        (layer_out, tokens_grad, keys_grad, w_in_grad, w_out_grad)
    )
    return layer_out, tokens_grad, keys_grad.T, w_in_grad[None], w_out_grad[None]


def solution(mesh):
    n_seq, n_exp = mesh.shape["seq"], mesh.shape["exp"]
    placed = (
        P(("seq", "exp"), None),
        P(None, "exp"),
        P("exp", "seq", None),
        P("exp", "seq", None),
        P(("seq", "exp"), None),
    )
    return jax.shard_map(
        functools.partial(local, n_seq, n_exp),
        mesh=mesh,
        in_specs=placed,
        out_specs=(
            P(("seq", "exp"), None),
            P(("seq", "exp"), None),
            P(None, "exp"),
            P("exp", "seq", None),
            P("exp", "seq", None),
        ),
        check_vma=False,
    )
```

```python
import functools

import jax
import jax.numpy as jnp
from jax import lax
from jax.experimental import pallas as pl
from jax.experimental.pallas import tpu as pltpu
from jax.sharding import PartitionSpec as P

tanh_coeff = 0.7978845608028654
cubic_coeff = 0.044715
F32 = jnp.float32
BF16 = jnp.bfloat16
MESH = pl.DeviceIdType.MESH
LANES = 128


def gelu_value(values):
    return (
        0.5
        * values
        * (1.0 + jnp.tanh(tanh_coeff * (values + cubic_coeff * values * values * values)))
    )


def gelu_slope(values):
    tanh_part = jnp.tanh(tanh_coeff * (values + cubic_coeff * values * values * values))
    return 0.5 * (1.0 + tanh_part) + 0.5 * values * (1.0 - tanh_part * tanh_part) * tanh_coeff * (
        1.0 + 3.0 * cubic_coeff * values * values
    )


def split_in_three(value):
    high = value.astype(BF16).astype(F32)
    rest = value - high
    middle = rest.astype(BF16).astype(F32)
    return high, middle, rest - middle


def packed_scalars(values):
    rows = values[0].shape[0]
    lane = lax.broadcasted_iota(jnp.int32, (rows, LANES), 1)
    result = jnp.zeros((rows, LANES), F32)
    at = 0
    for value in values:
        for part in split_in_three(value):
            result = jnp.where(lane == at, part, result)
            at += 1
    return result


def unpacked_scalars(row, count):
    lane = lax.broadcasted_iota(jnp.int32, row.shape, 1)
    found = []
    for k in range(count):
        mine = (lane >= 3 * k) & (lane < 3 * k + 3)
        found.append(jnp.sum(jnp.where(mine, row, 0.0), axis=1, keepdims=True))
    return found


def high_and_low(value):
    high = value.astype(BF16).astype(F32)
    return high, value - high


def dot(a, b, dims):
    return lax.dot_general(a, b, (dims, ((), ())), preferred_element_type=F32)


def farthest_first(n, over_exp):
    inner = 8 if over_exp and n % 8 == 0 else n

    def hops(k):
        near, far = k % inner, k // inner
        return min(near, inner - near) + min(far, n // inner - far)

    return sorted(range(1, n), key=lambda k: -hops(k))


def kernel(
    n_seq, n_exp, x_hbm, keys_hbm, w_in_hbm, w_out_hbm, c_hbm,
    layer_out, tokens_grad, keys_grad, w_in_grad, w_out_grad,
    x, keys_ref, c, w_in, w_out, k_all, so, sg, row_f, flat_f,
    a_buf, c1_send_in, c1_send_grad, c1_in, c1_grad, c2_in, c2_grad,
    e_out, e_grad, f_buf, h1_send, h1_buf, h2_buf,
    load_sem, send_sem, recv_sem,
):
    width = x.shape[1]
    blocks = width // LANES
    pairs = blocks // 2
    tall = blocks + 1
    s_me = lax.axis_index("seq")
    e_me = lax.axis_index("exp")

    loads = [
        pltpu.make_async_copy(source, target, load_sem.at[k])
        for k, (source, target) in enumerate(
            ((x_hbm, x), (c_hbm, c), (w_in_hbm, w_in), (w_out_hbm, w_out), (keys_hbm, keys_ref))
        )
    ]

    barrier = pltpu.get_barrier_semaphore()

    loads[4].start()
    for k in farthest_first(n_exp, True):
        pl.semaphore_signal(
            barrier, inc=1, device_id=(s_me, lax.rem(e_me + k, n_exp)), device_id_type=MESH
        )
    for k in farthest_first(n_seq, False):
        pl.semaphore_signal(
            barrier, inc=1, device_id=(lax.rem(s_me + k, n_seq), e_me), device_id_type=MESH
        )
    for load in loads[:4]:
        load.start()

    def exchange(over_exp, *parts):
        n, me = (n_exp, e_me) if over_exp else (n_seq, s_me)

        for k in farthest_first(n, over_exp):
            peer = lax.rem(me + k, n)
            target = (s_me, peer) if over_exp else (peer, e_me)
            for at, unit, source, buf in parts:
                mine = buf.at[pl.ds(me * unit, unit)]
                pltpu.make_async_remote_copy(
                    src_ref=mine if source is None else source.at[pl.ds(peer * unit, unit)],
                    dst_ref=mine,
                    send_sem=send_sem.at[at],
                    recv_sem=recv_sem.at[at],
                    device_id=target,
                    device_id_type=MESH,
                ).start()

    def whole(over_exp, at, unit, source, buf):
        n, me = (n_exp, e_me) if over_exp else (n_seq, s_me)
        peer = lax.rem(me + 1, n)
        every = buf.at[pl.ds(0, (n - 1) * unit)]
        return pltpu.make_async_remote_copy(
            src_ref=every,
            dst_ref=every,
            send_sem=send_sem.at[at],
            recv_sem=recv_sem.at[at],
            device_id=(s_me, peer) if over_exp else (peer, e_me),
            device_id_type=MESH,
        )

    started = []

    def begin(over_exp, *parts):
        exchange(over_exp, *parts)
        started.extend(whole(over_exp, *part) for part in parts)

        def arrived():
            for part in parts:
                whole(over_exp, *part).wait_recv()

        return arrived

    def cut(row):
        return [row[:, k * LANES : (k + 1) * LANES] for k in range(blocks)]

    def store_pairs(buf, me, rows):
        for k, row in enumerate(rows):
            row_f[pl.ds(k, 1), :] = row
        count = len(rows)
        unit = count // 2
        buf[pl.ds(me * unit, unit)] = row_f[0:count, :].reshape(unit, 2, LANES).astype(BF16)

    def store_rows(buf, me, unit, rows):
        for k, row in enumerate(rows):
            buf[pl.ds(me * unit + k, 1)] = row.reshape(1, 1, LANES)

    def load_pairs(buf):
        count = buf.shape[0] * 2
        flat_f[0:count, :] = buf.reshape(count, LANES)[...].astype(F32)

    def picked(source, row, count, rows):
        return source[pl.ds(row, count, stride=rows), :]

    def split_to(target, first, rows, values):
        for k in range(blocks):
            target[pl.ds(first + k, n_exp, stride=rows), :] = values[:, k * LANES : (k + 1) * LANES]

    lane = lax.broadcasted_iota(jnp.int32, (1, LANES), 1)

    def two_scalars(a, b):
        return jnp.where(lane < LANES // 2, a, b)

    loads[4].wait()
    store_pairs(a_buf, e_me, cut(keys_ref[...].astype(F32)))
    pl.semaphore_wait(barrier, n_exp - 1 + n_seq - 1)
    arrived = begin(True, (0, pairs, None, a_buf))
    loads[0].wait()
    loads[1].wait()
    arrived()
    load_pairs(a_buf)
    for k in range(blocks):
        k_all[:, k * LANES : (k + 1) * LANES] = picked(flat_f, k, n_exp, blocks).astype(BF16)

    logits = dot(k_all[...], x[...], ((1,), (1,)))
    local_peak = jnp.max(logits, axis=1, keepdims=True)
    local_terms = jnp.exp(logits - local_peak)
    local_total = jnp.sum(local_terms, axis=1, keepdims=True)
    row_peak = jnp.max(logits, axis=0, keepdims=True)
    row_terms = jnp.exp(logits - row_peak)
    comb_prob = row_terms / jnp.sum(row_terms, axis=0, keepdims=True)
    combine = comb_prob.astype(BF16)

    grad_view = c1_send_grad.reshape(n_exp * tall, LANES)
    grad_view[pl.ds(blocks, n_exp, stride=tall), :] = two_scalars(local_peak, local_total)
    split_to(grad_view, 0, tall, dot(combine, c[...], ((1,), (0,))))
    c1_grad[pl.ds(e_me * tall, tall)] = c1_send_grad[pl.ds(e_me * tall, tall)]
    arrived_grad = begin(True, (1, tall, c1_send_grad, c1_grad))
    both_terms = jnp.concatenate(high_and_low(local_terms), axis=0).astype(BF16)
    in_rows = dot(both_terms, x[...], ((1,), (0,)))
    split_to(flat_f, 0, blocks, in_rows[0:n_exp] + in_rows[n_exp:])
    c1_send_in.reshape(n_exp * blocks, LANES)[...] = flat_f[0 : n_exp * blocks, :].astype(BF16)
    c1_in[pl.ds(e_me * pairs, pairs)] = c1_send_in[pl.ds(e_me * pairs, pairs)]
    arrived_in = begin(True, (2, pairs, c1_send_in, c1_in))

    def summed(source, count, rows, scale=None):
        result = []
        for k in range(blocks):
            part = picked(source, k, count, rows)
            if scale is not None:
                part = part * scale
            result.append(jnp.sum(part, axis=0, keepdims=True))
        return result

    def merged_grad(buf, count):
        grad = buf.reshape(count * tall, LANES)
        stats = picked(grad, blocks, count, tall)
        peaks, totals = stats[:, 0:1], stats[:, LANES // 2 : LANES // 2 + 1]
        peak = jnp.max(peaks, axis=0, keepdims=True)
        scale = jnp.exp(peaks - peak)
        total = jnp.sum(scale * totals, axis=0, keepdims=True)
        return summed(grad, count, tall), peak, total, scale

    def merged_in(buf, count, scale):
        load_pairs(buf)
        return summed(flat_f, count, blocks, scale)

    arrived_grad()
    out_grad, peak, total, scale = merged_grad(c1_grad, n_exp)
    store_rows(c2_grad, s_me, tall, out_grad + [two_scalars(peak, total)])
    arrived_grad = begin(False, (3, tall, None, c2_grad))
    arrived_in()
    store_pairs(c2_in, s_me, merged_in(c1_in, n_exp, scale))
    arrived_in = begin(False, (4, pairs, None, c2_in))
    loads[2].wait()
    loads[3].wait()

    in_first = lax.broadcasted_iota(jnp.int32, (16, 1), 0) == 0

    def first_row(row):
        return jnp.where(in_first, row, 0.0).astype(BF16)

    def times(row, matrix, dim):
        return dot(row, matrix[...], ((1,), (dim,)))[0:1]

    arrived_grad()
    out_grad, slot_peak, slot_total, scale = merged_grad(c2_grad, n_seq)
    out_lhs = first_row(jnp.concatenate(out_grad, axis=1))
    act_grad = times(out_lhs, w_out, 1)
    arrived_in()
    slot_in = [part / slot_total for part in merged_in(c2_in, n_seq, scale)]
    in_lhs = first_row(jnp.concatenate(slot_in, axis=1))
    pre_act = times(in_lhs, w_in, 1)
    act_lhs = first_row(gelu_value(pre_act))
    pre_lhs = first_row(act_grad * gelu_slope(pre_act))
    slot_in_grad_part = times(pre_lhs, w_in, 0)
    slot_out_part = times(act_lhs, w_out, 0)

    store_rows(e_grad, s_me, blocks, cut(slot_in_grad_part))
    store_pairs(e_out, s_me, cut(slot_out_part))
    arrived = begin(False, (5, blocks, None, e_grad), (6, pairs, None, e_out))

    step = 2 * LANES
    for k in range(width // step):
        cols = slice(k * step, (k + 1) * step)
        w_out_grad[:, cols] = dot(act_lhs, out_lhs[:, cols], ((0,), (0,))).astype(BF16)
        w_in_grad[:, cols] = dot(pre_lhs, in_lhs[:, cols], ((0,), (0,))).astype(BF16)

    arrived()
    slot_in_grad = summed(e_grad.reshape(n_seq * blocks, LANES), n_seq, blocks)
    load_pairs(e_out)
    slot_out = summed(flat_f, n_seq, blocks)
    products = [a * b.astype(BF16).astype(F32) for a, b in zip(slot_in, slot_in_grad)]
    correction = jnp.sum(functools.reduce(jnp.add, products), axis=1, keepdims=True)

    both = 2 * (blocks + 1)
    scalars = packed_scalars((slot_peak, slot_total, correction))
    store_pairs(f_buf, e_me, slot_out + slot_in_grad + [scalars, jnp.zeros((1, LANES), F32)])
    arrived = begin(True, (7, both // 2, None, f_buf))
    arrived()
    load_pairs(f_buf)
    for k in range(blocks):
        cols = slice(k * LANES, (k + 1) * LANES)
        so[:, cols] = picked(flat_f, k, n_exp, both).astype(BF16)
        sg[:, cols] = picked(flat_f, blocks + k, n_exp, both).astype(BF16)
    peaks, totals, corrections = unpacked_scalars(picked(flat_f, 2 * blocks, n_exp, both), 3)

    comb_grad = dot(so[...], c[...], ((1,), (1,)))
    disp_grad = dot(sg[...], x[...], ((1,), (1,)))
    disp_prob = jnp.exp(logits - peaks) / totals
    comb_mean = jnp.sum(comb_prob * comb_grad, axis=0, keepdims=True)
    logit_grad = (
        comb_prob * (comb_grad - comb_mean) + disp_prob * (disp_grad - corrections)
    ).astype(BF16)

    split_to(flat_f, 0, blocks, dot(logit_grad, x[...], ((1,), (0,))))
    h1_send.reshape(n_exp * blocks, LANES)[...] = flat_f[0 : n_exp * blocks, :].astype(BF16)
    h1_buf[pl.ds(e_me * pairs, pairs)] = h1_send[pl.ds(e_me * pairs, pairs)]
    arrived = begin(True, (8, pairs, h1_send, h1_buf))

    layer_out[...] = dot(combine, so[...], ((0,), (0,))).astype(BF16)
    tokens_grad[...] = (
        dot(disp_prob.astype(BF16), sg[...], ((0,), (0,))) + dot(logit_grad, k_all[...], ((0,), (0,)))
    ).astype(BF16)

    arrived()
    load_pairs(h1_buf)
    store_pairs(h2_buf, s_me, summed(flat_f, n_exp, blocks))

    arrived = begin(False, (9, pairs, None, h2_buf))
    for copies in started:
        copies.wait_send()
    arrived()
    load_pairs(h2_buf)
    for k, part in enumerate(summed(flat_f, n_seq, blocks)):
        keys_grad[:, k * LANES : (k + 1) * LANES] = part


def put_kernel(*refs):
    count = (len(refs) - 1) // 2
    copies = []
    for k in range(count):
        rows = refs[k].shape[0]
        parts = 2 if rows % 32 == 0 else 1
        for part in range(parts):
            at = pl.ds(part * (rows // parts), rows // parts)
            copies.append(
                pltpu.make_async_copy(
                    refs[k].at[at], refs[count + k].at[at], refs[-1].at[2 * k + part]
                )
            )
    for copy in copies:
        copy.start()
    for copy in copies:
        copy.wait()


def put(arrays):
    count = len(arrays)
    return pl.pallas_call(
        put_kernel,
        out_shape=tuple(pltpu.HBM(a.shape, a.dtype) for a in arrays),
        in_specs=[pl.BlockSpec(memory_space=pltpu.VMEM)] * count,
        out_specs=(pl.BlockSpec(memory_space=pltpu.HBM),) * count,
        scratch_shapes=[pltpu.SemaphoreType.DMA((2 * count,))],
        compiler_params=pltpu.CompilerParams(vmem_limit_bytes=1024 * 1024),
        name="put",
    )(*arrays)


def local(n_seq, n_exp, tokens, slot_keys, w_in, w_out, cotangent):
    rows, width = tokens.shape
    hidden = w_in.shape[1]
    blocks = width // LANES
    pairs = blocks // 2
    tall = blocks + 1

    def pairs_of(count):
        return pltpu.VMEM((count, 2, LANES), BF16)

    def rows_of(count):
        return pltpu.VMEM((count, 1, LANES), F32)

    hbm = pl.BlockSpec(memory_space=pltpu.HBM)
    vmem = pl.BlockSpec(memory_space=pltpu.VMEM)
    layer_out, tokens_grad, keys_grad, w_in_grad, w_out_grad = pl.pallas_call(
        functools.partial(kernel, n_seq, n_exp),
        out_shape=(
            pltpu.VMEM((rows, width), BF16),
            pltpu.VMEM((rows, width), BF16),
            pltpu.VMEM((1, width), F32),
            pltpu.VMEM((hidden, width), BF16),
            pltpu.VMEM((hidden, width), BF16),
        ),
        in_specs=[hbm, hbm, hbm, hbm, hbm],
        out_specs=(vmem, vmem, vmem, vmem, vmem),
        scratch_shapes=[
            pltpu.VMEM((rows, width), BF16),
            pltpu.VMEM((1, width), BF16),
            pltpu.VMEM((rows, width), BF16),
            pltpu.VMEM((hidden, width), BF16),
            pltpu.VMEM((hidden, width), BF16),
            pltpu.VMEM((n_exp, width), BF16),
            pltpu.VMEM((n_exp, width), BF16),
            pltpu.VMEM((n_exp, width), BF16),
            pltpu.VMEM((2 * tall, LANES), F32),
            pltpu.VMEM((max(n_seq, n_exp) * 2 * tall, LANES), F32),
            pairs_of(n_exp * pairs),
            pairs_of(n_exp * pairs),
            rows_of(n_exp * tall),
            pairs_of(n_exp * pairs),
            rows_of(n_exp * tall),
            pairs_of(n_seq * pairs),
            rows_of(n_seq * tall),
            pairs_of(n_seq * pairs),
            rows_of(n_seq * blocks),
            pairs_of(n_exp * tall),
            pairs_of(n_exp * pairs),
            pairs_of(n_exp * pairs),
            pairs_of(n_seq * pairs),
            pltpu.SemaphoreType.DMA((5,)),
            pltpu.SemaphoreType.DMA((10,)),
            pltpu.SemaphoreType.DMA((10,)),
        ],
        compiler_params=pltpu.CompilerParams(
            collective_id=0, has_side_effects=True, vmem_limit_bytes=32 * 1024 * 1024
        ),
        name="moe",
    )(
        *(
            pltpu.with_memory_space_constraint(a, pltpu.HBM)
            for a in (tokens, slot_keys.T, w_in[0], w_out[0], cotangent)
        )
    )
    layer_out, tokens_grad, keys_grad, w_in_grad, w_out_grad = put(
        (layer_out, tokens_grad, keys_grad, w_in_grad, w_out_grad)
    )
    return layer_out, tokens_grad, keys_grad.T, w_in_grad[None], w_out_grad[None]


def solution(mesh):
    n_seq, n_exp = mesh.shape["seq"], mesh.shape["exp"]
    placed = (
        P(("seq", "exp"), None),
        P(None, "exp"),
        P("exp", "seq", None),
        P("exp", "seq", None),
        P(("seq", "exp"), None),
    )
    return jax.shard_map(
        functools.partial(local, n_seq, n_exp),
        mesh=mesh,
        in_specs=placed,
        out_specs=(
            P(("seq", "exp"), None),
            P(("seq", "exp"), None),
            P(None, "exp"),
            P("exp", "seq", None),
            P("exp", "seq", None),
        ),
        check_vma=False,
    )
```

```python
import functools

import jax
import jax.numpy as jnp
from jax import lax
from jax.experimental import pallas as pl
from jax.experimental.pallas import tpu as pltpu
from jax.sharding import PartitionSpec as P

tanh_coeff = 0.7978845608028654
cubic_coeff = 0.044715
F32 = jnp.float32
BF16 = jnp.bfloat16
MESH = pl.DeviceIdType.MESH
LANES = 128


def gelu_value(values):
    return (
        0.5
        * values
        * (1.0 + jnp.tanh(tanh_coeff * (values + cubic_coeff * values * values * values)))
    )


def gelu_slope(values):
    tanh_part = jnp.tanh(tanh_coeff * (values + cubic_coeff * values * values * values))
    return 0.5 * (1.0 + tanh_part) + 0.5 * values * (1.0 - tanh_part * tanh_part) * tanh_coeff * (
        1.0 + 3.0 * cubic_coeff * values * values
    )


def split_in_three(value):
    high = value.astype(BF16).astype(F32)
    rest = value - high
    middle = rest.astype(BF16).astype(F32)
    return high, middle, rest - middle


def packed_scalars(values):
    rows = values[0].shape[0]
    lane = lax.broadcasted_iota(jnp.int32, (rows, LANES), 1)
    result = jnp.zeros((rows, LANES), F32)
    at = 0
    for value in values:
        for part in split_in_three(value):
            result = jnp.where(lane == at, part, result)
            at += 1
    return result


def unpacked_scalars(row, count):
    lane = lax.broadcasted_iota(jnp.int32, row.shape, 1)
    found = []
    for k in range(count):
        mine = (lane >= 3 * k) & (lane < 3 * k + 3)
        found.append(jnp.sum(jnp.where(mine, row, 0.0), axis=1, keepdims=True))
    return found


def dot(a, b, dims):
    return lax.dot_general(a, b, (dims, ((), ())), preferred_element_type=F32)


def farthest_first(n, over_exp):
    inner = 8 if over_exp and n % 8 == 0 else n

    def hops(k):
        near, far = k % inner, k // inner
        return min(near, inner - near) + min(far, n // inner - far)

    return sorted(range(1, n), key=lambda k: -hops(k))


def kernel(
    n_seq, n_exp, x_hbm, keys_hbm, w_in_hbm, w_out_hbm, c_hbm,
    layer_out, tokens_grad, keys_grad, w_in_grad, w_out_grad,
    x, keys_ref, c, w_in, w_out, k_all, so, sg, row_f, flat_f,
    a_buf, c1_send_in, c1_send_grad, c1_in, c1_grad, c2_in, c2_grad,
    e_out, e_grad, f_buf, h1_send, h1_buf, h2_buf,
    load_sem, send_sem, recv_sem,
):
    width = x.shape[1]
    blocks = width // LANES
    pairs = blocks // 2
    tall = blocks + 1
    s_me = lax.axis_index("seq")
    e_me = lax.axis_index("exp")

    loads = [
        pltpu.make_async_copy(source, target, load_sem.at[k])
        for k, (source, target) in enumerate(
            ((x_hbm, x), (c_hbm, c), (w_in_hbm, w_in), (w_out_hbm, w_out), (keys_hbm, keys_ref))
        )
    ]

    barrier = pltpu.get_barrier_semaphore()

    loads[4].start()
    for k in farthest_first(n_exp, True):
        pl.semaphore_signal(
            barrier, inc=1, device_id=(s_me, lax.rem(e_me + k, n_exp)), device_id_type=MESH
        )
    for k in farthest_first(n_seq, False):
        pl.semaphore_signal(
            barrier, inc=1, device_id=(lax.rem(s_me + k, n_seq), e_me), device_id_type=MESH
        )
    for load in loads[:4]:
        load.start()

    def exchange(over_exp, *parts):
        n, me = (n_exp, e_me) if over_exp else (n_seq, s_me)

        for k in farthest_first(n, over_exp):
            peer = lax.rem(me + k, n)
            target = (s_me, peer) if over_exp else (peer, e_me)
            for at, unit, source, buf in parts:
                mine = buf.at[pl.ds(me * unit, unit)]
                pltpu.make_async_remote_copy(
                    src_ref=mine if source is None else source.at[pl.ds(peer * unit, unit)],
                    dst_ref=mine,
                    send_sem=send_sem.at[at],
                    recv_sem=recv_sem.at[at],
                    device_id=target,
                    device_id_type=MESH,
                ).start()

    def whole(over_exp, at, unit, source, buf):
        n, me = (n_exp, e_me) if over_exp else (n_seq, s_me)
        peer = lax.rem(me + 1, n)
        every = buf.at[pl.ds(0, (n - 1) * unit)]
        return pltpu.make_async_remote_copy(
            src_ref=every,
            dst_ref=every,
            send_sem=send_sem.at[at],
            recv_sem=recv_sem.at[at],
            device_id=(s_me, peer) if over_exp else (peer, e_me),
            device_id_type=MESH,
        )

    started = []

    def begin(over_exp, *parts):
        exchange(over_exp, *parts)
        started.extend(whole(over_exp, *part) for part in parts)

        def arrived():
            for part in parts:
                whole(over_exp, *part).wait_recv()

        return arrived

    def cut(row):
        return [row[:, k * LANES : (k + 1) * LANES] for k in range(blocks)]

    def store_pairs(buf, me, rows):
        for k, row in enumerate(rows):
            row_f[pl.ds(k, 1), :] = row
        count = len(rows)
        unit = count // 2
        buf[pl.ds(me * unit, unit)] = row_f[0:count, :].reshape(unit, 2, LANES).astype(BF16)

    def store_rows(buf, me, unit, rows):
        for k, row in enumerate(rows):
            buf[pl.ds(me * unit + k, 1)] = row.reshape(1, 1, LANES)

    def load_pairs(buf):
        count = buf.shape[0] * 2
        flat_f[0:count, :] = buf.reshape(count, LANES)[...].astype(F32)

    def picked(source, row, count, rows):
        return source[pl.ds(row, count, stride=rows), :]

    def split_to(target, first, rows, values):
        for k in range(blocks):
            target[pl.ds(first + k, n_exp, stride=rows), :] = values[:, k * LANES : (k + 1) * LANES]

    lane = lax.broadcasted_iota(jnp.int32, (1, LANES), 1)

    def two_scalars(a, b):
        return jnp.where(lane < LANES // 2, a, b)

    loads[4].wait()
    store_pairs(a_buf, e_me, cut(keys_ref[...].astype(F32)))
    pl.semaphore_wait(barrier, n_exp - 1 + n_seq - 1)
    arrived = begin(True, (0, pairs, None, a_buf))
    loads[0].wait()
    loads[1].wait()
    arrived()
    load_pairs(a_buf)
    for k in range(blocks):
        k_all[:, k * LANES : (k + 1) * LANES] = picked(flat_f, k, n_exp, blocks).astype(BF16)

    logits = dot(k_all[...], x[...], ((1,), (1,)))
    local_peak = jnp.max(logits, axis=1, keepdims=True)
    local_terms = jnp.exp(logits - local_peak)
    local_total = jnp.sum(local_terms, axis=1, keepdims=True)
    row_peak = jnp.max(logits, axis=0, keepdims=True)
    row_terms = jnp.exp(logits - row_peak)
    comb_prob = row_terms / jnp.sum(row_terms, axis=0, keepdims=True)
    combine = comb_prob.astype(BF16)

    grad_view = c1_send_grad.reshape(n_exp * tall, LANES)
    grad_view[pl.ds(blocks, n_exp, stride=tall), :] = two_scalars(local_peak, local_total)
    split_to(grad_view, 0, tall, dot(combine, c[...], ((1,), (0,))))
    c1_grad[pl.ds(e_me * tall, tall)] = c1_send_grad[pl.ds(e_me * tall, tall)]
    arrived_grad = begin(True, (1, tall, c1_send_grad, c1_grad))
    split_to(flat_f, 0, blocks, dot(local_terms.astype(BF16), x[...], ((1,), (0,))))
    c1_send_in.reshape(n_exp * blocks, LANES)[...] = flat_f[0 : n_exp * blocks, :].astype(BF16)
    c1_in[pl.ds(e_me * pairs, pairs)] = c1_send_in[pl.ds(e_me * pairs, pairs)]
    arrived_in = begin(True, (2, pairs, c1_send_in, c1_in))

    def summed(source, count, rows, scale=None):
        result = []
        for k in range(blocks):
            part = picked(source, k, count, rows)
            if scale is not None:
                part = part * scale
            result.append(jnp.sum(part, axis=0, keepdims=True))
        return result

    def merged_grad(buf, count):
        grad = buf.reshape(count * tall, LANES)
        stats = picked(grad, blocks, count, tall)
        peaks, totals = stats[:, 0:1], stats[:, LANES // 2 : LANES // 2 + 1]
        peak = jnp.max(peaks, axis=0, keepdims=True)
        scale = jnp.exp(peaks - peak)
        total = jnp.sum(scale * totals, axis=0, keepdims=True)
        return summed(grad, count, tall), peak, total, scale

    def merged_in(buf, count, scale):
        load_pairs(buf)
        return summed(flat_f, count, blocks, scale)

    arrived_grad()
    out_grad, peak, total, scale = merged_grad(c1_grad, n_exp)
    store_rows(c2_grad, s_me, tall, out_grad + [two_scalars(peak, total)])
    arrived_grad = begin(False, (3, tall, None, c2_grad))
    arrived_in()
    store_pairs(c2_in, s_me, merged_in(c1_in, n_exp, scale))
    arrived_in = begin(False, (4, pairs, None, c2_in))
    loads[2].wait()
    loads[3].wait()

    in_first = lax.broadcasted_iota(jnp.int32, (16, 1), 0) == 0

    def first_row(row):
        return jnp.where(in_first, row, 0.0).astype(BF16)

    def times(row, matrix, dim):
        return dot(row, matrix[...], ((1,), (dim,)))[0:1]

    arrived_grad()
    out_grad, slot_peak, slot_total, scale = merged_grad(c2_grad, n_seq)
    out_lhs = first_row(jnp.concatenate(out_grad, axis=1))
    act_grad = times(out_lhs, w_out, 1)
    arrived_in()
    slot_in = [part / slot_total for part in merged_in(c2_in, n_seq, scale)]
    in_lhs = first_row(jnp.concatenate(slot_in, axis=1))
    pre_act = times(in_lhs, w_in, 1)
    act_lhs = first_row(gelu_value(pre_act))
    pre_lhs = first_row(act_grad * gelu_slope(pre_act))
    slot_in_grad_part = times(pre_lhs, w_in, 0)
    slot_out_part = times(act_lhs, w_out, 0)

    store_rows(e_grad, s_me, blocks, cut(slot_in_grad_part))
    store_pairs(e_out, s_me, cut(slot_out_part))
    arrived = begin(False, (5, blocks, None, e_grad), (6, pairs, None, e_out))

    step = 2 * LANES
    for k in range(width // step):
        cols = slice(k * step, (k + 1) * step)
        w_out_grad[:, cols] = dot(act_lhs, out_lhs[:, cols], ((0,), (0,))).astype(BF16)
        w_in_grad[:, cols] = dot(pre_lhs, in_lhs[:, cols], ((0,), (0,))).astype(BF16)

    arrived()
    slot_in_grad = summed(e_grad.reshape(n_seq * blocks, LANES), n_seq, blocks)
    load_pairs(e_out)
    slot_out = summed(flat_f, n_seq, blocks)
    products = [a * b.astype(BF16).astype(F32) for a, b in zip(slot_in, slot_in_grad)]
    correction = jnp.sum(functools.reduce(jnp.add, products), axis=1, keepdims=True)

    both = 2 * (blocks + 1)
    scalars = packed_scalars((slot_peak, slot_total, correction))
    store_pairs(f_buf, e_me, slot_out + slot_in_grad + [scalars, jnp.zeros((1, LANES), F32)])
    arrived = begin(True, (7, both // 2, None, f_buf))
    arrived()
    load_pairs(f_buf)
    for k in range(blocks):
        cols = slice(k * LANES, (k + 1) * LANES)
        so[:, cols] = picked(flat_f, k, n_exp, both).astype(BF16)
        sg[:, cols] = picked(flat_f, blocks + k, n_exp, both).astype(BF16)
    peaks, totals, corrections = unpacked_scalars(picked(flat_f, 2 * blocks, n_exp, both), 3)

    comb_grad = dot(so[...], c[...], ((1,), (1,)))
    disp_grad = dot(sg[...], x[...], ((1,), (1,)))
    disp_prob = jnp.exp(logits - peaks) / totals
    comb_mean = jnp.sum(comb_prob * comb_grad, axis=0, keepdims=True)
    logit_grad = (
        comb_prob * (comb_grad - comb_mean) + disp_prob * (disp_grad - corrections)
    ).astype(BF16)

    split_to(flat_f, 0, blocks, dot(logit_grad, x[...], ((1,), (0,))))
    h1_send.reshape(n_exp * blocks, LANES)[...] = flat_f[0 : n_exp * blocks, :].astype(BF16)
    h1_buf[pl.ds(e_me * pairs, pairs)] = h1_send[pl.ds(e_me * pairs, pairs)]
    arrived = begin(True, (8, pairs, h1_send, h1_buf))

    layer_out[...] = dot(combine, so[...], ((0,), (0,))).astype(BF16)
    tokens_grad[...] = (
        dot(disp_prob.astype(BF16), sg[...], ((0,), (0,))) + dot(logit_grad, k_all[...], ((0,), (0,)))
    ).astype(BF16)

    arrived()
    load_pairs(h1_buf)
    store_pairs(h2_buf, s_me, summed(flat_f, n_exp, blocks))

    arrived = begin(False, (9, pairs, None, h2_buf))
    for copies in started:
        copies.wait_send()
    arrived()
    load_pairs(h2_buf)
    for k, part in enumerate(summed(flat_f, n_seq, blocks)):
        keys_grad[:, k * LANES : (k + 1) * LANES] = part


def put_kernel(*refs):
    count = (len(refs) - 1) // 2
    copies = [
        pltpu.make_async_copy(refs[k], refs[count + k], refs[-1].at[k]) for k in range(count)
    ]
    for copy in copies:
        copy.start()
    for copy in copies:
        copy.wait()


def put(arrays):
    count = len(arrays)
    return pl.pallas_call(
        put_kernel,
        out_shape=tuple(pltpu.HBM(a.shape, a.dtype) for a in arrays),
        in_specs=[pl.BlockSpec(memory_space=pltpu.VMEM)] * count,
        out_specs=(pl.BlockSpec(memory_space=pltpu.HBM),) * count,
        scratch_shapes=[pltpu.SemaphoreType.DMA((count,))],
        compiler_params=pltpu.CompilerParams(vmem_limit_bytes=1024 * 1024),
        name="put",
    )(*arrays)


def local(n_seq, n_exp, tokens, slot_keys, w_in, w_out, cotangent):
    rows, width = tokens.shape
    hidden = w_in.shape[1]
    blocks = width // LANES
    pairs = blocks // 2
    tall = blocks + 1

    def pairs_of(count):
        return pltpu.VMEM((count, 2, LANES), BF16)

    def rows_of(count):
        return pltpu.VMEM((count, 1, LANES), F32)

    hbm = pl.BlockSpec(memory_space=pltpu.HBM)
    vmem = pl.BlockSpec(memory_space=pltpu.VMEM)
    layer_out, tokens_grad, keys_grad, w_in_grad, w_out_grad = pl.pallas_call(
        functools.partial(kernel, n_seq, n_exp),
        out_shape=(
            pltpu.VMEM((rows, width), BF16),
            pltpu.VMEM((rows, width), BF16),
            pltpu.VMEM((1, width), F32),
            pltpu.VMEM((hidden, width), BF16),
            pltpu.VMEM((hidden, width), BF16),
        ),
        in_specs=[hbm, hbm, hbm, hbm, hbm],
        out_specs=(vmem, vmem, vmem, vmem, vmem),
        scratch_shapes=[
            pltpu.VMEM((rows, width), BF16),
            pltpu.VMEM((1, width), BF16),
            pltpu.VMEM((rows, width), BF16),
            pltpu.VMEM((hidden, width), BF16),
            pltpu.VMEM((hidden, width), BF16),
            pltpu.VMEM((n_exp, width), BF16),
            pltpu.VMEM((n_exp, width), BF16),
            pltpu.VMEM((n_exp, width), BF16),
            pltpu.VMEM((2 * tall, LANES), F32),
            pltpu.VMEM((max(n_seq, n_exp) * 2 * tall, LANES), F32),
            pairs_of(n_exp * pairs),
            pairs_of(n_exp * pairs),
            rows_of(n_exp * tall),
            pairs_of(n_exp * pairs),
            rows_of(n_exp * tall),
            pairs_of(n_seq * pairs),
            rows_of(n_seq * tall),
            pairs_of(n_seq * pairs),
            rows_of(n_seq * blocks),
            pairs_of(n_exp * tall),
            pairs_of(n_exp * pairs),
            pairs_of(n_exp * pairs),
            pairs_of(n_seq * pairs),
            pltpu.SemaphoreType.DMA((5,)),
            pltpu.SemaphoreType.DMA((10,)),
            pltpu.SemaphoreType.DMA((10,)),
        ],
        compiler_params=pltpu.CompilerParams(
            collective_id=0, has_side_effects=True, vmem_limit_bytes=32 * 1024 * 1024
        ),
        name="moe",
    )(
        *(
            pltpu.with_memory_space_constraint(a, pltpu.HBM)
            for a in (tokens, slot_keys.T, w_in[0], w_out[0], cotangent)
        )
    )
    layer_out, tokens_grad, keys_grad, w_in_grad, w_out_grad = put(
        (layer_out, tokens_grad, keys_grad, w_in_grad, w_out_grad)
    )
    return layer_out, tokens_grad, keys_grad.T, w_in_grad[None], w_out_grad[None]


def solution(mesh):
    n_seq, n_exp = mesh.shape["seq"], mesh.shape["exp"]
    placed = (
        P(("seq", "exp"), None),
        P(None, "exp"),
        P("exp", "seq", None),
        P("exp", "seq", None),
        P(("seq", "exp"), None),
    )
    return jax.shard_map(
        functools.partial(local, n_seq, n_exp),
        mesh=mesh,
        in_specs=placed,
        out_specs=(
            P(("seq", "exp"), None),
            P(("seq", "exp"), None),
            P(None, "exp"),
            P("exp", "seq", None),
            P("exp", "seq", None),
        ),
        check_vma=False,
    )
```
